256 devices in a mesh: seq: 32 (over y, x, core), head: 8 (over z).
Axes of the slice: x: 4, y: 4, z: 8, core: 2. Of those that a mesh axis runs over, the one named last changes fastest.
Arguments:
- old_cache: bfloat16 [2048, 8, 128, 128], P(('seq', 'head')), may hold values from -9 to 9
- page_dest: int32 [2048], P(('seq', 'head')), may hold values from 0 to 2047, as said below
- seq_pages: int32 [64], replicated, may hold values from 1 to 128, 2048 in all
- last_fill: int32 [64], replicated, may hold values from 1 to 128
- queries: bfloat16 [64, 8, 512], P(None, 'head'), may hold values from -16 to 16
Outputs:
- new_cache: bfloat16 [2048, 8, 128, 128], P('seq', 'head')
- attended: bfloat16 [64, 8, 512], P('seq', 'head')
The draws below stay inside these ranges and needn't reach their ends.
Inputs may be any that keep to these rules, and one draw needn't show every extreme that they name: page_dest is a permutation of the page numbers. The 64 old pages p with the same p // 64 go to exactly 16 distinct new owners page_dest[p] // 64, exactly 4 pages to each; every new owner receives 64 pages.
All inputs are finite; a program needn't handle non-finite values.
Results may differ from the reference program's by a relative error of at most 0.004.
Values may be sent and summed in bfloat16 or wider, within the bound.
A program may use at most 64 MiB of HBM per device.

```python
import math
import jax
import jax.numpy as jnp
import numpy as np
from jax import lax

KVH = 8
GROUP = 8
HD = 64
PAGE = 128
PAGES_DEV = 64
PAGES_ALL = 2048
SEQS = 64
MOST = 128
ROUTES = 16
CAP = 4
N_SEQ = 32
N_HEAD = 8


def draw_old_cache(key, part):
    key_first, key_second = jax.random.split(jax.random.fold_in(key, 11), 2)
    full_shape = (PAGES_ALL, KVH, PAGE, HD)
    key_part = jax.random.truncated_normal(key_first, -4.5, 4.5, full_shape, jnp.float32)
    value_part = jax.random.truncated_normal(key_second, -4.5, 4.5, full_shape, jnp.float32)
    return jnp.concatenate([key_part, value_part], axis=-1).astype(jnp.bfloat16)


def draw_queries(key, part):
    key_first = jax.random.fold_in(jax.random.fold_in(key, 23), 0)
    query_noise = 2.5 * jax.random.truncated_normal(key_first, -4.0, 4.0, (SEQS, KVH, GROUP, HD), jnp.float32)
    return query_noise.reshape(SEQS, KVH, GROUP * HD).astype(jnp.bfloat16)


def draw_page_dest(key, part):
    key_offsets, key_spans, key_pages, key_slots = jax.random.split(jax.random.fold_in(key, 37), 4)
    per_old = PAGES_DEV // N_HEAD
    offsets = jax.random.permutation(key_offsets, N_SEQ)[:ROUTES]
    span_order = jax.vmap(lambda subkey: jax.random.permutation(subkey, ROUTES))(jax.random.split(key_spans, N_SEQ))
    shuffles = jax.vmap(lambda subkey: jax.random.permutation(subkey, per_old))(jax.random.split(key_pages, N_SEQ * N_HEAD))
    slot_order = jax.vmap(lambda subkey: jax.random.permutation(subkey, PAGES_DEV))(jax.random.split(key_slots, N_SEQ))
    page_ids = jnp.arange(PAGES_ALL, dtype=jnp.int32)
    device_old = page_ids // per_old
    row_index = page_ids // PAGES_DEV
    within = page_ids % per_old
    position = shuffles[device_old, within]
    span_index = device_old % N_HEAD * (per_old // CAP) + position // CAP
    route_index = span_order[row_index, span_index]
    target = (row_index + offsets[route_index]) % N_SEQ
    slot_index = slot_order[target, route_index * CAP + position % CAP]
    return (target * PAGES_DEV + slot_index).astype(jnp.int32)


def with_ends(entries, own_key, smallest, high):
    longest = entries.shape.index(max(entries.shape))
    spots = []
    for shift in (0, 1):
        where = [jax.random.randint(jax.random.fold_in(own_key, axis), (), 0, length) for axis, length in enumerate(entries.shape)]
        where[longest] = (where[longest] + shift) % entries.shape[longest]
        spots.append(tuple(where))
    return entries.at[spots[0]].set(smallest).at[spots[1]].set(high)


def profile(number_of, total, limit, lean):
    loads = [(1 << 20) // math.isqrt(rank ** lean) + 1 for rank in range(2, number_of + 1)]
    surplus, counts = total - limit - (number_of - 1), [1] * (number_of - 1)
    while surplus > 0:
        free = [i for i in range(number_of - 1) if counts[i] < limit]
        whole, remaining = sum([loads[i] for i in free]), surplus
        for i in free:
            extra = min(limit - counts[i], max(1, remaining * loads[i] // whole), surplus)
            counts[i] = counts[i] + extra
            surplus = surplus - extra
    return np.array([limit] + counts)


def uneven(own_key, number_of, total, bound, slope):
    if number_of == 2:
        one = jax.random.randint(own_key, (), max(1, total - bound), min(bound, total - 1) + 1)
        return jnp.stack([one, total - one])
    sizes = jnp.asarray(profile(number_of, total, bound, slope), jnp.int32)
    twos = (number_of - 1) // 2
    giver, receiver = sizes[1:1 + 2 * twos:2], sizes[2:2 + 2 * twos:2]
    slack = jnp.minimum(giver - 1, bound - receiver)
    moved = jax.random.randint(jax.random.fold_in(own_key, 1), (twos,), 0, 1 << 20) % (slack + 1)
    sizes = sizes.at[1:1 + 2 * twos:2].set(giver - moved).at[2:2 + 2 * twos:2].set(receiver + moved)
    return sizes[jax.random.permutation(jax.random.fold_in(own_key, 2), number_of)]


def setup_inputs(seed: int = 0) -> dict:
    splits = jax.random.split(jax.random.key(seed), 6)
    return {
        "old_cache": draw_old_cache(jax.random.fold_in(splits[5], 71), 0),
        "page_dest": draw_page_dest(jax.random.fold_in(splits[5], 71), 0),
        "seq_pages": uneven(splits[2], SEQS, PAGES_ALL, MOST, 2).astype(jnp.int32),
        "last_fill": with_ends(jax.random.randint(splits[3], (SEQS,), 1, PAGE + 1), jax.random.fold_in(splits[3], 1), 1, PAGE).astype(jnp.int32),
        "queries": draw_queries(jax.random.fold_in(splits[5], 71), 0),
    }


NEG_FILL = -1.0e30


def reference(old_cache, page_dest, seq_pages, last_fill, queries):
    new_cache = jnp.zeros_like(old_cache).at[page_dest].set(old_cache)
    page_ids = jnp.arange(PAGES_ALL, dtype=jnp.int32)
    position = ((page_ids % PAGES_DEV) * N_SEQ + page_ids // PAGES_DEV).astype(jnp.int32)
    seq_ends = jnp.cumsum(seq_pages).astype(jnp.int32)
    page_owner = jnp.sum((position[:, None] >= seq_ends[None, :]).astype(jnp.int32), axis=1).astype(jnp.int32)
    member = page_owner[None, :] == jnp.arange(SEQS, dtype=jnp.int32)[:, None]
    owner_end = jnp.take(seq_ends, page_owner)
    owner_fill = jnp.take(last_fill, page_owner)
    page_fill = jnp.where(position == owner_end - 1, owner_fill, PAGE)
    token_live = jnp.arange(PAGE, dtype=jnp.int32)[None, :] < page_fill[:, None]
    scale_factor = HD ** -0.5
    member_float = member.astype(jnp.float32)

    def one_head(operands):
        head_cache, head_query = operands
        page_query = jnp.take(head_query, page_owner, axis=0).astype(jnp.float32).reshape(PAGES_ALL, GROUP, HD)
        key_part = head_cache[:, :, :HD].astype(jnp.float32)
        value_part = head_cache[:, :, HD:].astype(jnp.float32)
        scores = jnp.einsum("pgd,ptd->pgt", page_query, key_part, precision=lax.Precision.HIGHEST) * scale_factor
        scores = jnp.where(token_live[:, None, :], scores, NEG_FILL)
        page_max = jnp.max(scores, axis=2)
        seq_max = jnp.max(jnp.where(member[:, :, None], page_max[None, :, :], NEG_FILL), axis=1)
        owner_max = jnp.take(seq_max, page_owner, axis=0)
        weights = jnp.where(token_live[:, None, :], jnp.exp(scores - owner_max[:, :, None]), 0.0).astype(jnp.bfloat16)
        weights = lax.optimization_barrier(weights).astype(jnp.float32)
        page_total = jnp.sum(weights, axis=2)
        page_sum = jnp.einsum("pgt,ptd->pgd", weights, value_part, precision=lax.Precision.HIGHEST)
        totals = jnp.dot(member_float, page_total, precision=lax.Precision.HIGHEST)
        weighted = jnp.dot(member_float, page_sum.reshape(PAGES_ALL, GROUP * HD), precision=lax.Precision.HIGHEST)
        result = weighted.reshape(SEQS, GROUP, HD) / totals[:, :, None]
        return result.reshape(SEQS, GROUP * HD)

    head_first = jnp.moveaxis(new_cache, 1, 0)
    attended = lax.map(one_head, (head_first, jnp.moveaxis(queries, 1, 0)))
    attended = jnp.moveaxis(attended, 0, 1).astype(jnp.bfloat16)
    return new_cache, attended
```

```python
import functools

import jax
import jax.numpy as jnp
from jax import lax
from jax.experimental import pallas as pl
from jax.experimental.pallas import tpu as pltpu
from jax.sharding import PartitionSpec as P

NEG_FILL = -1e30
CHUNKS = 8
TOK = 16
LANES = 128
MESH = pl.DeviceIdType.MESH

CHIP_ORDER = (
    (1, 2), (2, 3), (3, 2), (2, 1), (1, 1), (3, 3), (0, 2), (2, 0),
    (1, 3), (3, 1), (2, 2), (0, 1), (1, 0), (0, 3), (3, 0),
)
PEERS = tuple((y, x, c) for c in (0, 1) for y, x in CHIP_ORDER) + ((0, 0, 1),)
HEAD_ORDER = (4, 3, 5, 2, 6, 1, 7)


def iota(shape, dim):
    return lax.broadcasted_iota(jnp.int32, shape, dim)


def seq_peer(seq, offset):
    dy, dx, dc = offset
    y, x, c = seq // 8, (seq // 2) % 4, seq % 2
    return ((y + dy) % 4) * 8 + ((x + dx) % 4) * 2 + (c + dc) % 2


def remote(src, dst, send_sem, recv_sem, device):
    return pltpu.make_async_remote_copy(
        src_ref=src, dst_ref=dst, send_sem=send_sem, recv_sem=recv_sem,
        device_id=device, device_id_type=MESH,
    )


def wait_bytes(ref, sem):
    pltpu.make_async_copy(ref, ref, sem).wait()


def kernel(
    old_hbm, dest_s, meta_v, q3, out_v, att_v,
    old_v, dst_v, lab_out, lab_in, tab_v, tab_s, tab2_v, tab2_s,
    fill_v, memb_v, sc_v, m_v, o_v, c_v, rj_v, r4_v, rb_v, regs, outgs, incs,
    zs, zr, xs, xr, ds, dr, ls, lr, ps, pr, ld, tsem, t2sem,
):
    h = lax.axis_index("head")
    s = lax.axis_index("seq")
    n_head, n_seq = 8, 32

    load = pltpu.make_async_copy(old_hbm, old_v, ld)
    load.start()
    bar = pltpu.get_barrier_semaphore()

    @pl.loop(1, n_head)
    def _(d):
        pl.semaphore_signal(bar, inc=1, device_id={"head": (h + d) % n_head}, device_id_type=MESH)

    @pl.loop(1, n_seq)
    def _(d):
        pl.semaphore_signal(bar, inc=1, device_id={"seq": (s + d) % n_seq}, device_id_type=MESH)

    own = pl.ds(pl.multiple_of(h * 8, 8), 8)
    row8 = iota((8, LANES), 0)
    mine = jnp.zeros((8, LANES), jnp.int32)
    for i in range(8):
        mine = jnp.where(row8 == i, dest_s[i], mine)
    dst_v[own, :] = mine

    sub, lane = iota((LANES, LANES), 0), iota((LANES, LANES), 1)
    pages_row = meta_v[0:1, :]
    fill_row = meta_v[1:2, :]
    pages_t = jnp.broadcast_to(pages_row, (LANES, LANES)).T
    end_row = jnp.sum(jnp.where(sub <= lane, pages_t, 0), axis=0, keepdims=True)
    start_row = end_row - pages_row

    pl.semaphore_wait(bar, n_head - 1 + n_seq - 1)

    for d in HEAD_ORDER:
        k = (h + d) % n_head
        remote(dst_v.at[own], dst_v.at[own], ds, dr, {"head": k}).start()
    load.wait()
    for c in range(CHUNKS):
        for d in HEAD_ORDER:
            k = (h + d) % n_head
            remote(
                old_v.at[:, k, pl.ds(c * TOK, TOK), :], regs[c].at[own], zs.at[c], zr.at[c], {"head": k}
            ).start()
    for c in range(CHUNKS):
        regs[c][own] = old_v[:, h, pl.ds(c * TOK, TOK), :]

    wait_bytes(dst_v.at[pl.ds(0, 56)], dr)
    row, col = iota((64, LANES), 0), iota((64, LANES), 1)
    dest = dst_v[...]
    target, slot = dest >> 6, dest & 63
    chosen = (target == (col >> 2)).astype(jnp.int32)
    count = chosen
    for k in (1, 2, 4, 8, 16, 32):
        count = count + jnp.where(row >= k, pltpu.roll(count, k, 0), 0)
    picked = (chosen > 0) & ((count - chosen) == (col & 3))
    src_row = jnp.sum(jnp.where(picked, row, 0), axis=0, keepdims=True)
    lab_row = jnp.sum(jnp.where(picked, slot + 1, 0), axis=0, keepdims=True) - 1
    lab_out[...] = jnp.broadcast_to(lab_row, (LANES, LANES)).T
    place = slot * n_seq + target
    member = (place >= start_row) & (place < end_row)
    owner = jnp.sum(jnp.where(member, col, 0), axis=1, keepdims=True)
    owner = jnp.broadcast_to(owner, (64, LANES))
    owner_row = jnp.concatenate([owner, owner], axis=0).T[0:1, :]
    last = member & (place == end_row - 1)
    fill = jnp.sum(jnp.where(last, fill_row - LANES, 0), axis=1, keepdims=True) + LANES
    fill_v[...] = jnp.broadcast_to(fill, (64, LANES))
    memb_v[...] = member.astype(jnp.float32)
    tab_v[0:1, :] = jnp.minimum(src_row, 63)
    tab_v[1:2, :] = jnp.minimum(owner_row, 63)
    table = pltpu.make_async_copy(tab_v, tab_s, tsem)
    table.start()
    mine8 = pl.ds(pl.multiple_of(s * 8, 8), 8)
    for o in PEERS:
        t = seq_peer(s, o)
        remote(
            lab_out.at[pl.ds(pl.multiple_of((t // 2) * 8, 8), 8)], lab_in.at[mine8], ls, lr, {"seq": t}
        ).start()
    lab_in[mine8, :] = lab_out[pl.ds(pl.multiple_of((s // 2) * 8, 8), 8), :]
    table.wait()

    def anchors():
        wait_bytes(lab_in.at[pl.ds(0, 248)], lr)
        r, g = iota((256, LANES), 0), iota((256, LANES), 1)
        hit = (lab_in[...] == g) & (((r & 7) >> 2) == s % 2)
        place = jnp.sum(jnp.where(hit, (r >> 3) * 4 + (r & 3), 0), axis=0, keepdims=True)
        tab2_v[0:1, :] = jnp.minimum(place, LANES - 1)
        back = pltpu.make_async_copy(tab2_v, tab2_s, t2sem)
        back.start()
        back.wait()

    def put(c):
        wait_bytes(incs[c].at[pl.ds(0, 124)], xr.at[c])

        @pl.loop(0, 64, unroll=8)
        def _(g):
            out_v[g, pl.ds(c * TOK, TOK), :] = incs[c][tab2_s[0, g]]

    mine4 = pl.ds(s * 4, 4)
    for c in range(CHUNKS):
        wait_bytes(regs[c].at[pl.ds(0, 56)], zr.at[c])

        @pl.loop(0, LANES, unroll=8)
        def _(i):
            outgs[c][i] = regs[c][tab_s[0, i]]

        for o in PEERS:
            t = seq_peer(s, o)
            remote(outgs[c].at[pl.ds(t * 4, 4)], incs[c].at[mine4], xs.at[c], xr.at[c], {"seq": t}).start()
        incs[c][mine4] = outgs[c][mine4]
        if c == 1:
            anchors()
        if c >= 2:
            put(c - 2)

    lane8 = iota((8, LANES), 1)

    def page_rows(p):
        return pl.ds(pl.multiple_of(p * 8, 8), 8)

    def page_kv(p):
        return jnp.concatenate([regs[c][p] for c in range(CHUNKS)], axis=0)

    @pl.loop(0, 64, unroll=8)
    def _(p):
        q = q3[tab_s[1, p]].astype(jnp.bfloat16)
        score = lax.dot_general(
            q, page_kv(p), (((1,), (1,)), ((), ())), preferred_element_type=jnp.float32
        ) * 0.125
        score = jnp.where(lane8 < fill_v[pl.ds(p, 1), :], score, NEG_FILL)
        sc_v[page_rows(p), :] = score

    def seq_max_step(p, best):
        top = jnp.broadcast_to(jnp.max(sc_v[page_rows(p), :], axis=1, keepdims=True), (8, LANES))
        m_v[page_rows(p), :] = top
        return jnp.maximum(best, jnp.where(memb_v[pl.ds(p, 1), :] > 0, top, NEG_FILL))

    best = lax.fori_loop(0, 64, seq_max_step, jnp.full((8, LANES), NEG_FILL, jnp.float32), unroll=8)

    @pl.loop(0, 64, unroll=8)
    def _(p):
        top = m_v[page_rows(p), :]
        weights = jnp.exp(sc_v[page_rows(p), :] - top).astype(jnp.bfloat16)
        total = jnp.sum(weights.astype(jnp.float32), axis=1, keepdims=True)
        summed = lax.dot_general(
            weights, page_kv(p), (((1,), (0,)), ((), ())), preferred_element_type=jnp.float32
        )
        o_v[page_rows(p), :] = jnp.where(lane8 < 64, total, summed)
        c_v[page_rows(p), :] = jnp.where(memb_v[pl.ds(p, 1), :] > 0, jnp.exp(top - best), 0.0)

    best_t = jnp.concatenate([best] * 16, axis=0).T
    lane64 = iota((64, LANES), 1)
    for j in range(8):
        coef = c_v[pl.ds(j, 64, stride=8), :]
        sums = o_v[pl.ds(j, 64, stride=8), :]
        res = lax.dot_general(
            coef.T, sums, (((1,), (0,)), ((), ())),
            precision=lax.Precision.HIGHEST, preferred_element_type=jnp.float32,
        )[0:64, :]
        tops = best_t[0:64, j : j + 1]
        rj_v[j] = jnp.where((lane64 >= 32) & (lane64 < 64), tops, res)
        for b in range(2):
            r4_v[pl.ds(j * 2 + b, 32, stride=16), :] = rj_v[j, pl.ds(b, 32, stride=2), :]

    mine16 = pl.ds(pl.multiple_of(s * 16, 16), 16)
    for o in PEERS:
        t = seq_peer(s, o)
        remote(
            r4_v.at[pl.ds(pl.multiple_of(t * 16, 16), 16)], rb_v.at[mine16], ps, pr, {"seq": t}
        ).start()
    rb_v[mine16, :] = r4_v[mine16, :]

    put(CHUNKS - 2)
    put(CHUNKS - 1)

    wait_bytes(rb_v.at[pl.ds(0, 496)], pr)
    parts = rb_v[...].reshape(n_seq, 16, LANES)
    tops = jnp.broadcast_to(parts[:, :, 32:33], (n_seq, 16, LANES))
    scaled = jnp.exp(tops - jnp.max(tops, axis=0, keepdims=True)) * parts
    acc = jnp.sum(scaled, axis=0)
    att_v[...] = acc / acc[:, 0:1]

    wait_bytes(dst_v.at[pl.ds(0, 56)], ds)
    wait_bytes(lab_in.at[pl.ds(0, 248)], ls)
    wait_bytes(rb_v.at[pl.ds(0, 496)], ps)
    for c in range(CHUNKS):
        wait_bytes(regs[c].at[pl.ds(0, 56)], zs.at[c])
        wait_bytes(incs[c].at[pl.ds(0, 124)], xs.at[c])


def per_device(old_cache, page_dest, seq_pages, last_fill, queries):
    meta = jnp.stack([jnp.pad(seq_pages, (0, 64)), jnp.pad(last_fill, (0, 64))])
    q3 = jnp.pad(queries.reshape(64, 8, 64).astype(jnp.float32), ((0, 0), (0, 0), (0, 64)))
    bf, f32, i32 = jnp.bfloat16, jnp.float32, jnp.int32
    vmem, dma = pltpu.VMEM, pltpu.SemaphoreType.DMA
    new_cache, att = pl.pallas_call(
        kernel,
        out_shape=(
            jax.ShapeDtypeStruct((64, 128, 128), bf),
            jax.ShapeDtypeStruct((16, LANES), f32),
        ),
        in_specs=[
            pl.BlockSpec(memory_space=pl.ANY),
            pl.BlockSpec(memory_space=pltpu.SMEM),
            pl.BlockSpec(memory_space=pltpu.VMEM),
            pl.BlockSpec(memory_space=pltpu.VMEM),
        ],
        out_specs=(pl.BlockSpec(memory_space=pltpu.VMEM), pl.BlockSpec(memory_space=pltpu.VMEM)),
        scratch_shapes=[
            vmem((8, 8, 128, 128), bf),
            vmem((64, LANES), i32),
            vmem((LANES, LANES), i32),
            vmem((256, LANES), i32),
            vmem((8, LANES), i32),
            pltpu.SMEM((8, LANES), i32),
            vmem((8, LANES), i32),
            pltpu.SMEM((8, LANES), i32),
            vmem((64, LANES), i32),
            vmem((64, LANES), f32),
            vmem((512, LANES), f32),
            vmem((512, LANES), f32),
            vmem((512, LANES), f32),
            vmem((512, LANES), f32),
            vmem((8, 64, LANES), f32),
            vmem((512, LANES), f32),
            vmem((512, LANES), f32),
            [vmem((64, TOK, LANES), bf)] * CHUNKS,
            [vmem((128, TOK, LANES), bf)] * CHUNKS,
            [vmem((128, TOK, LANES), bf)] * CHUNKS,
            dma((CHUNKS,)), dma((CHUNKS,)), dma((CHUNKS,)), dma((CHUNKS,)),
            dma, dma, dma, dma, dma, dma, dma, dma, dma,
        ],
        compiler_params=pltpu.CompilerParams(
            collective_id=0, has_side_effects=True, vmem_limit_bytes=40 * 2**20
        ),
    )(old_cache, page_dest, meta, q3)
    attended = att.reshape(8, 2, LANES)[:, :, 64:].transpose(1, 0, 2).reshape(2, 1, 512)
    return new_cache.reshape(64, 1, 128, 128), attended.astype(bf)


def solution(mesh):
    in_specs = (
        P(("seq", "head"), None, None, None),
        P(("seq", "head")),
        P(),
        P(),
        P(None, "head", None),
    )
    out_specs = (P("seq", "head", None, None), P("seq", "head", None))
    return jax.shard_map(
        per_device, mesh=mesh, in_specs=in_specs, out_specs=out_specs, check_vma=False
    )
```

```python
import functools

import jax
import jax.numpy as jnp
from jax import lax
from jax.experimental import pallas as pl
from jax.experimental.pallas import tpu as pltpu
from jax.sharding import PartitionSpec as P

NEG_FILL = -1e30
CHUNKS = 16
TOK = 8
LAG = 3
LANES = 128
MESH = pl.DeviceIdType.MESH

CHIP_ORDER = (
    (1, 2), (2, 3), (3, 2), (2, 1), (1, 1), (3, 3), (0, 2), (2, 0),
    (1, 3), (3, 1), (2, 2), (0, 1), (1, 0), (0, 3), (3, 0),
)
PEERS = tuple((y, x, c) for c in (0, 1) for y, x in CHIP_ORDER) + ((0, 0, 1),)
HEAD_ORDER = (4, 3, 5, 2, 6, 1, 7)


def iota(shape, dim):
    return lax.broadcasted_iota(jnp.int32, shape, dim)


def seq_peer(seq, offset):
    dy, dx, dc = offset
    y, x, c = seq // 8, (seq // 2) % 4, seq % 2
    return ((y + dy) % 4) * 8 + ((x + dx) % 4) * 2 + (c + dc) % 2


def remote(src, dst, send_sem, recv_sem, device):
    return pltpu.make_async_remote_copy(
        src_ref=src, dst_ref=dst, send_sem=send_sem, recv_sem=recv_sem,
        device_id=device, device_id_type=MESH,
    )


def wait_bytes(ref, sem):
    pltpu.make_async_copy(ref, ref, sem).wait()


def kernel(
    old_hbm, dest_hbm, pages_hbm, fill_hbm, q_hbm, out_v, att_v,
    old_v, q_v, q3, kv_v, dest_s, pages_s, last_s, dst_v, lab_out, lab_in, tab_v, tab_s, tab2_v, tab2_s,
    fill_v, memb_v, m_v, o_v, c_v, rj_v, bt_v, ro_v, rm_v, po_v, pm_v, regs, outgs, incs,
    zs, zr, xs, xr, ds, dr, ls, lr, ps, pr, ms, mr, ld, sd, tsem, t2sem,
):
    h = lax.axis_index("head")
    s = lax.axis_index("seq")
    n_head, n_seq = 8, 32

    small = [
        pltpu.make_async_copy(src, dst, sd.at[i])
        for i, (src, dst) in enumerate(
            ((dest_hbm, dest_s), (pages_hbm, pages_s), (fill_hbm, last_s), (q_hbm, q_v))
        )
    ]
    load = pltpu.make_async_copy(old_hbm, old_v, ld)
    for copy in small:
        copy.start()
    load.start()
    bar = pltpu.get_barrier_semaphore()

    @pl.loop(1, n_head)
    def _(d):
        pl.semaphore_signal(bar, inc=1, device_id={"head": (h + d) % n_head}, device_id_type=MESH)

    @pl.loop(1, n_seq)
    def _(d):
        pl.semaphore_signal(bar, inc=1, device_id={"seq": (s + d) % n_seq}, device_id_type=MESH)

    for copy in small:
        copy.wait()
    own = pl.ds(pl.multiple_of(h * 8, 8), 8)
    row8 = iota((8, LANES), 0)
    mine = jnp.zeros((8, LANES), jnp.int32)
    for i in range(8):
        mine = jnp.where(row8 == i, dest_s[i], mine)
    dst_v[own, :] = mine

    lane1 = iota((1, LANES), 1)
    start_row = jnp.full((1, LANES), 1 << 20, jnp.int32)
    end_row, fill_row = start_row, jnp.zeros((1, LANES), jnp.int32)
    end = jnp.int32(0)
    for k in range(64):
        start_row = jnp.where(lane1 == k, end, start_row)
        end = end + pages_s[k]
        end_row = jnp.where(lane1 == k, end, end_row)
        fill_row = jnp.where(lane1 == k, last_s[k], fill_row)
    lane64 = iota((64, LANES), 1)
    for j in range(8):
        pair = q_v[:, (j // 2) * LANES : (j // 2 + 1) * LANES].astype(jnp.float32)
        if j % 2:
            pair = pltpu.roll(pair, 64, 1)
        q3[:, j, :] = jnp.where(lane64 < 64, pair, 0.0)

    pl.semaphore_wait(bar, n_head - 1 + n_seq - 1)

    for d in HEAD_ORDER:
        k = (h + d) % n_head
        remote(dst_v.at[own], dst_v.at[own], ds, dr, {"head": k}).start()
    load.wait()
    for c in range(CHUNKS):
        for d in HEAD_ORDER:
            k = (h + d) % n_head
            remote(
                old_v.at[:, k, pl.ds(c * TOK, TOK), :], regs[c].at[own], zs.at[c], zr.at[c], {"head": k}
            ).start()
    for c in range(CHUNKS):
        regs[c][own] = old_v[:, h, pl.ds(c * TOK, TOK), :]

    wait_bytes(dst_v.at[pl.ds(0, 56)], dr)
    row, col = iota((64, LANES), 0), iota((64, LANES), 1)
    dest = dst_v[...]
    target, slot = dest >> 6, dest & 63
    chosen = (target == (col >> 2)).astype(jnp.int32)
    count = chosen
    for k in (1, 2, 4, 8, 16, 32):
        count = count + jnp.where(row >= k, pltpu.roll(count, k, 0), 0)
    picked = (chosen > 0) & ((count - chosen) == (col & 3))
    src_row = jnp.sum(jnp.where(picked, row, 0), axis=0, keepdims=True)
    lab_row = jnp.sum(jnp.where(picked, slot + 1, 0), axis=0, keepdims=True) - 1
    lab_out[...] = jnp.broadcast_to(lab_row, (LANES, LANES)).T
    place = slot * n_seq + target
    member = (place >= start_row) & (place < end_row)
    owner = jnp.sum(jnp.where(member, col, 0), axis=1, keepdims=True)
    owner = jnp.broadcast_to(owner, (64, LANES))
    owner_row = jnp.concatenate([owner, owner], axis=0).T[0:1, :]
    last = member & (place == end_row - 1)
    fill = jnp.sum(jnp.where(last, fill_row - LANES, 0), axis=1, keepdims=True) + LANES
    fill_v[...] = jnp.broadcast_to(fill, (64, LANES))
    memb_v[...] = member.astype(jnp.float32)
    tab_v[0:1, :] = jnp.minimum(src_row, 63)
    tab_v[1:2, :] = jnp.minimum(owner_row, 63)
    table = pltpu.make_async_copy(tab_v, tab_s, tsem)
    table.start()
    mine8 = pl.ds(pl.multiple_of(s * 8, 8), 8)
    for o in PEERS:
        t = seq_peer(s, o)
        remote(
            lab_out.at[pl.ds(pl.multiple_of((t // 2) * 8, 8), 8)], lab_in.at[mine8], ls, lr, {"seq": t}
        ).start()
    lab_in[mine8, :] = lab_out[pl.ds(pl.multiple_of((s // 2) * 8, 8), 8), :]
    table.wait()

    def anchors():
        wait_bytes(lab_in.at[pl.ds(0, 248)], lr)
        r, g = iota((256, LANES), 0), iota((256, LANES), 1)
        hit = (lab_in[...] == g) & (((r & 7) >> 2) == s % 2)
        place = jnp.sum(jnp.where(hit, (r >> 3) * 4 + (r & 3), 0), axis=0, keepdims=True)
        tab2_v[0:1, :] = jnp.minimum(place, LANES - 1)
        back = pltpu.make_async_copy(tab2_v, tab2_s, t2sem)
        back.start()
        back.wait()

    def put(c):
        wait_bytes(incs[c].at[pl.ds(0, 124)], xr.at[c])

        @pl.loop(0, 64, unroll=8)
        def _(g):
            out_v[g, pl.ds(c * TOK, TOK), :] = incs[c][tab2_s[0, g]]

    lane8 = iota((8, LANES), 1)
    lane_half = iota((8, 64), 1)

    def page_rows(p):
        return pl.ds(pl.multiple_of(p * 8, 8), 8)

    def attend(half, groups):
        tokens = pl.ds(half * 64, 64)
        for group in groups:
            pages = range(group * 8, group * 8 + 8)
            scores = []
            for p in pages:
                q = q3[tab_s[1, p]].astype(jnp.bfloat16)
                score = lax.dot_general(
                    q, kv_v[p, tokens, :], (((1,), (1,)), ((), ())), preferred_element_type=jnp.float32
                ) * 0.125
                scores.append(jnp.where(lane_half + half * 64 < fill_v[pl.ds(p, 1), 0:64], score, NEG_FILL))
            for p, score in zip(pages, scores):
                top = jnp.max(score, axis=1, keepdims=True)
                weights = jnp.exp(score - top).astype(jnp.bfloat16)
                total = jnp.sum(weights.astype(jnp.float32), axis=1, keepdims=True)
                summed = lax.dot_general(
                    weights, kv_v[p, tokens, :], (((1,), (0,)), ((), ())), preferred_element_type=jnp.float32
                )
                rows = page_rows(half * 64 + p)
                m_v[rows, :] = jnp.broadcast_to(top, (8, LANES))
                o_v[rows, :] = jnp.where(lane8 < 64, total, summed)

    mine4 = pl.ds(s * 4, 4)
    for c in range(CHUNKS):
        wait_bytes(regs[c].at[pl.ds(0, 56)], zr.at[c])

        @pl.loop(0, LANES, unroll=8)
        def _(i):
            outgs[c][i] = regs[c][tab_s[0, i]]

        for o in PEERS:
            t = seq_peer(s, o)
            remote(outgs[c].at[pl.ds(t * 4, 4)], incs[c].at[mine4], xs.at[c], xr.at[c], {"seq": t}).start()
        incs[c][mine4] = outgs[c][mine4]
        kv_v[:, pl.ds(c * TOK, TOK), :] = regs[c][...]
        if c == LAG - 1:
            anchors()
        if c >= LAG:
            put(c - LAG)
        if c >= CHUNKS // 2:
            attend(0, range(c - CHUNKS // 2, c - CHUNKS // 2 + 1))

    attend(1, range(8))
    best = jnp.full((8, LANES), NEG_FILL, jnp.float32)

    def seq_max_step(p, best):
        top = jnp.maximum(m_v[page_rows(p), :], m_v[page_rows(64 + p), :])
        return jnp.maximum(best, jnp.where(memb_v[pl.ds(p, 1), :] > 0, top, NEG_FILL))

    best = lax.fori_loop(0, 64, seq_max_step, best, unroll=16)

    @pl.loop(0, 64, unroll=16)
    def _(p):
        inside = memb_v[pl.ds(p, 1), :] > 0
        for half in range(2):
            rows = page_rows(half * 64 + p)
            c_v[rows, :] = jnp.where(inside, jnp.exp(m_v[rows, :] - best), 0.0)

    bt_v[...] = jnp.concatenate([best] * 16, axis=0).T
    lane32 = iota((32, LANES), 1)
    stats = jnp.zeros((32, LANES), jnp.float32)
    for b in range(2):
        stats = jnp.where(
            (lane32 >> 3) == 2 + b, bt_v[pl.ds(b, 32, stride=2), :], stats
        )
    for j in range(8):
        coef = c_v[pl.ds(j, 128, stride=8), :]
        sums = o_v[pl.ds(j, 128, stride=8), :]
        rj_v[j] = lax.dot_general(
            coef.T, sums, (((1,), (0,)), ((), ())),
            precision=lax.Precision.HIGHEST, preferred_element_type=jnp.float32,
        )[0:64, :]
        even, odd = rj_v[j, pl.ds(0, 32, stride=2), :], rj_v[j, pl.ds(1, 32, stride=2), :]
        stats = jnp.where(lane32 == j, even[:, 0:1], stats)
        stats = jnp.where(lane32 == 8 + j, odd[:, 0:1], stats)
        ro_v[pl.ds(j, 32, stride=8), :] = jnp.where(lane32 < 64, pltpu.roll(even, 64, 1), odd)
    rm_v[:, 0, :] = stats

    for o in PEERS:
        t = seq_peer(s, o)
        remote(
            ro_v.at[pl.ds(pl.multiple_of(t * 8, 8), 8)], po_v.at[mine8], ps, pr, {"seq": t}
        ).start()
        remote(rm_v.at[t], pm_v.at[s], ms, mr, {"seq": t}).start()
    po_v[mine8, :] = ro_v[mine8, :]
    pm_v[s] = rm_v[s]

    for c in range(CHUNKS - LAG, CHUNKS):
        put(c)

    wait_bytes(pm_v.at[pl.ds(0, 31)], mr)
    turned = jnp.concatenate([pm_v[:, 0, :]] * 4, axis=0).T
    totals, tops = turned[0:16, :], turned[16:32, :]
    coef = jnp.exp(tops - jnp.max(tops, axis=1, keepdims=True))
    total = jnp.sum(jnp.where(iota((16, LANES), 1) < n_seq, coef * totals, 0.0), axis=1, keepdims=True)
    coef = coef / total
    wait_bytes(po_v.at[pl.ds(0, 248)], pr)
    acc = jnp.zeros((8, LANES), jnp.float32)
    for t in range(n_seq):
        part = jnp.where(lane8 < 64, coef[0:8, t : t + 1], coef[8:16, t : t + 1])
        acc = acc + part * po_v[t * 8 : (t + 1) * 8, :]
    att_v[...] = acc

    wait_bytes(dst_v.at[pl.ds(0, 56)], ds)
    wait_bytes(lab_in.at[pl.ds(0, 248)], ls)
    wait_bytes(po_v.at[pl.ds(0, 248)], ps)
    wait_bytes(pm_v.at[pl.ds(0, 31)], ms)
    for c in range(CHUNKS):
        wait_bytes(regs[c].at[pl.ds(0, 56)], zs.at[c])
        wait_bytes(incs[c].at[pl.ds(0, 124)], xs.at[c])


def per_device(old_cache, page_dest, seq_pages, last_fill, queries):
    bf, f32, i32 = jnp.bfloat16, jnp.float32, jnp.int32
    vmem, dma = pltpu.VMEM, pltpu.SemaphoreType.DMA
    new_cache, att = pl.pallas_call(
        kernel,
        out_shape=(
            jax.ShapeDtypeStruct((64, 128, 128), bf),
            jax.ShapeDtypeStruct((8, LANES), f32),
        ),
        in_specs=[pl.BlockSpec(memory_space=pltpu.HBM)] * 5,
        out_specs=(pl.BlockSpec(memory_space=pltpu.VMEM), pl.BlockSpec(memory_space=pltpu.VMEM)),
        scratch_shapes=[
            vmem((8, 8, 128, 128), bf),
            vmem((64, 512), bf),
            vmem((64, 8, LANES), f32),
            vmem((64, 128, 128), bf),
            pltpu.SMEM((8,), i32),
            pltpu.SMEM((64,), i32),
            pltpu.SMEM((64,), i32),
            vmem((64, LANES), i32),
            vmem((LANES, LANES), i32),
            vmem((256, LANES), i32),
            vmem((8, LANES), i32),
            pltpu.SMEM((8, LANES), i32),
            vmem((8, LANES), i32),
            pltpu.SMEM((8, LANES), i32),
            vmem((64, LANES), i32),
            vmem((64, LANES), f32),
            vmem((1024, LANES), f32),
            vmem((1024, LANES), f32),
            vmem((1024, LANES), f32),
            vmem((8, 64, LANES), f32),
            vmem((LANES, LANES), f32),
            vmem((256, LANES), f32),
            vmem((32, 1, LANES), f32),
            vmem((256, LANES), f32),
            vmem((32, 1, LANES), f32),
            [vmem((64, TOK, LANES), bf)] * CHUNKS,
            [vmem((128, TOK, LANES), bf)] * CHUNKS,
            [vmem((128, TOK, LANES), bf)] * CHUNKS,
            dma((CHUNKS,)), dma((CHUNKS,)), dma((CHUNKS,)), dma((CHUNKS,)),
            dma, dma, dma, dma, dma, dma, dma, dma, dma, dma((4,)), dma, dma,
        ],
        compiler_params=pltpu.CompilerParams(
            collective_id=0, has_side_effects=True, vmem_limit_bytes=50 * 2**20
        ),
    )(*[pltpu.with_memory_space_constraint(x, pltpu.HBM) for x in (old_cache, page_dest, seq_pages, last_fill, queries.reshape(64, 512))])
    attended = att.reshape(8, 2, 64).transpose(1, 0, 2).reshape(2, 1, 512)
    return new_cache.reshape(64, 1, 128, 128), attended.astype(bf)


def solution(mesh):
    in_specs = (
        P(("seq", "head"), None, None, None),
        P(("seq", "head")),
        P(),
        P(),
        P(None, "head", None),
    )
    out_specs = (P("seq", "head", None, None), P("seq", "head", None))
    return jax.shard_map(
        per_device, mesh=mesh, in_specs=in_specs, out_specs=out_specs, check_vma=False
    )
```

```python
import functools

import jax
import jax.numpy as jnp
from jax import lax
from jax.experimental import pallas as pl
from jax.experimental.pallas import tpu as pltpu
from jax.sharding import PartitionSpec as P

NEG_FILL = -1e30
CHUNKS = 16
TOK = 8
LAG = 4
LANES = 128
MESH = pl.DeviceIdType.MESH

CHIP_ORDER = (
    (1, 2), (2, 3), (3, 2), (2, 1), (1, 1), (3, 3), (0, 2), (2, 0),
    (1, 3), (3, 1), (2, 2), (0, 1), (1, 0), (0, 3), (3, 0),
)
PEERS = tuple((y, x, c) for c in (0, 1) for y, x in CHIP_ORDER) + ((0, 0, 1),)
HEAD_ORDER = (4, 3, 5, 2, 6, 1, 7)


def iota(shape, dim):
    return lax.broadcasted_iota(jnp.int32, shape, dim)


def seq_peer(seq, offset):
    dy, dx, dc = offset
    y, x, c = seq // 8, (seq // 2) % 4, seq % 2
    return ((y + dy) % 4) * 8 + ((x + dx) % 4) * 2 + (c + dc) % 2


def remote(src, dst, send_sem, recv_sem, device):
    return pltpu.make_async_remote_copy(
        src_ref=src, dst_ref=dst, send_sem=send_sem, recv_sem=recv_sem,
        device_id=device, device_id_type=MESH,
    )


def wait_bytes(ref, sem):
    pltpu.make_async_copy(ref, ref, sem).wait()


def kernel(
    old_hbm, dest_hbm, pages_hbm, fill_hbm, q_hbm, out_v, att_v,
    old_v, q_v, q3, kv_v, dest_s, pages_s, last_s, dst_v, lab_out, lab_in, tab_v, tab_s, tab2_v, tab2_s,
    fill_v, memb_v, m_v, o_v, c_v, rj_v, bt_v, ro_v, rm_v, po_v, pm_v, regs, outgs, incs,
    zs, zr, xs, xr, ds, dr, ls, lr, ps, pr, ms, mr, ld, sd, tsem, t2sem,
):
    h = lax.axis_index("head")
    s = lax.axis_index("seq")
    n_head, n_seq = 8, 32

    small = [
        pltpu.make_async_copy(src, dst, sd.at[i])
        for i, (src, dst) in enumerate(
            ((dest_hbm, dest_s), (pages_hbm, pages_s), (fill_hbm, last_s), (q_hbm, q_v))
        )
    ]
    load = pltpu.make_async_copy(old_hbm, old_v, ld)
    for copy in small:
        copy.start()
    load.start()
    bar = pltpu.get_barrier_semaphore()

    @pl.loop(1, n_head)
    def _(d):
        pl.semaphore_signal(bar, inc=1, device_id={"head": (h + d) % n_head}, device_id_type=MESH)

    @pl.loop(1, n_seq)
    def _(d):
        pl.semaphore_signal(bar, inc=1, device_id={"seq": (s + d) % n_seq}, device_id_type=MESH)

    small[0].wait()
    own = pl.ds(pl.multiple_of(h * 8, 8), 8)
    row8 = iota((8, LANES), 0)
    mine = jnp.zeros((8, LANES), jnp.int32)
    for i in range(8):
        mine = jnp.where(row8 == i, dest_s[i], mine)
    dst_v[own, :] = mine

    pl.semaphore_wait(bar, n_head - 1 + n_seq - 1)

    for d in HEAD_ORDER:
        k = (h + d) % n_head
        remote(dst_v.at[own], dst_v.at[own], ds, dr, {"head": k}).start()
    load.wait()
    for c in range(CHUNKS):
        for d in HEAD_ORDER:
            k = (h + d) % n_head
            remote(
                old_v.at[:, k, pl.ds(c * TOK, TOK), :], regs[c].at[own], zs.at[c], zr.at[c], {"head": k}
            ).start()
    for c in range(CHUNKS):
        regs[c][own] = old_v[:, h, pl.ds(c * TOK, TOK), :]

    for copy in small[1:]:
        copy.wait()
    lane1 = iota((1, LANES), 1)
    start_row = jnp.full((1, LANES), 1 << 20, jnp.int32)
    end_row, fill_row = start_row, jnp.zeros((1, LANES), jnp.int32)
    end = jnp.int32(0)
    for k in range(64):
        start_row = jnp.where(lane1 == k, end, start_row)
        end = end + pages_s[k]
        end_row = jnp.where(lane1 == k, end, end_row)
        fill_row = jnp.where(lane1 == k, last_s[k], fill_row)
    lane64 = iota((64, LANES), 1)
    for j in range(8):
        pair = q_v[:, (j // 2) * LANES : (j // 2 + 1) * LANES].astype(jnp.float32)
        if j % 2:
            pair = pltpu.roll(pair, 64, 1)
        q3[:, j, :] = jnp.where(lane64 < 64, pair, 0.0)

    wait_bytes(dst_v.at[pl.ds(0, 56)], dr)
    row, col = iota((64, LANES), 0), iota((64, LANES), 1)
    dest = dst_v[...]
    target, slot = dest >> 6, dest & 63
    chosen = (target == (col >> 2)).astype(jnp.int32)
    count = chosen
    for k in (1, 2, 4, 8, 16, 32):
        count = count + jnp.where(row >= k, pltpu.roll(count, k, 0), 0)
    picked = (chosen > 0) & ((count - chosen) == (col & 3))
    src_row = jnp.sum(jnp.where(picked, row, 0), axis=0, keepdims=True)
    lab_row = jnp.sum(jnp.where(picked, slot + 1, 0), axis=0, keepdims=True) - 1
    lab_out[...] = jnp.broadcast_to(lab_row, (LANES, LANES)).T
    place = slot * n_seq + target
    member = (place >= start_row) & (place < end_row)
    owner = jnp.sum(jnp.where(member, col, 0), axis=1, keepdims=True)
    owner = jnp.broadcast_to(owner, (64, LANES))
    owner_row = jnp.concatenate([owner, owner], axis=0).T[0:1, :]
    last = member & (place == end_row - 1)
    fill = jnp.sum(jnp.where(last, fill_row - LANES, 0), axis=1, keepdims=True) + LANES
    fill_v[...] = jnp.broadcast_to(fill, (64, LANES))
    memb_v[...] = member.astype(jnp.float32)
    tab_v[0:1, :] = jnp.minimum(src_row, 63)
    tab_v[1:2, :] = jnp.minimum(owner_row, 63)
    table = pltpu.make_async_copy(tab_v, tab_s, tsem)
    table.start()
    mine8 = pl.ds(pl.multiple_of(s * 8, 8), 8)
    for o in PEERS:
        t = seq_peer(s, o)
        remote(
            lab_out.at[pl.ds(pl.multiple_of((t // 2) * 8, 8), 8)], lab_in.at[mine8], ls, lr, {"seq": t}
        ).start()
    lab_in[mine8, :] = lab_out[pl.ds(pl.multiple_of((s // 2) * 8, 8), 8), :]
    table.wait()

    def anchors():
        wait_bytes(lab_in.at[pl.ds(0, 248)], lr)
        r, g = iota((256, LANES), 0), iota((256, LANES), 1)
        hit = (lab_in[...] == g) & (((r & 7) >> 2) == s % 2)
        place = jnp.sum(jnp.where(hit, (r >> 3) * 4 + (r & 3), 0), axis=0, keepdims=True)
        tab2_v[0:1, :] = jnp.minimum(place, LANES - 1)
        back = pltpu.make_async_copy(tab2_v, tab2_s, t2sem)
        back.start()
        back.wait()

    def put(c):
        wait_bytes(incs[c].at[pl.ds(0, 124)], xr.at[c])

        @pl.loop(0, 64, unroll=8)
        def _(g):
            out_v[g, pl.ds(c * TOK, TOK), :] = incs[c][tab2_s[0, g]]

    lane8 = iota((8, LANES), 1)
    lane_half = iota((8, 64), 1)

    def page_rows(p):
        return pl.ds(pl.multiple_of(p * 8, 8), 8)

    def attend(half, groups):
        tokens = pl.ds(half * 64, 64)
        for group in groups:
            pages = range(group * 8, group * 8 + 8)
            scores = []
            for p in pages:
                q = q3[tab_s[1, p]].astype(jnp.bfloat16)
                score = lax.dot_general(
                    q, kv_v[p, tokens, :], (((1,), (1,)), ((), ())), preferred_element_type=jnp.float32
                ) * 0.125
                scores.append(jnp.where(lane_half + half * 64 < fill_v[pl.ds(p, 1), 0:64], score, NEG_FILL))
            for p, score in zip(pages, scores):
                top = jnp.max(score, axis=1, keepdims=True)
                weights = jnp.exp(score - top).astype(jnp.bfloat16)
                total = jnp.sum(weights.astype(jnp.float32), axis=1, keepdims=True)
                summed = lax.dot_general(
                    weights, kv_v[p, tokens, :], (((1,), (0,)), ((), ())), preferred_element_type=jnp.float32
                )
                rows = page_rows(half * 64 + p)
                m_v[rows, :] = jnp.broadcast_to(top, (8, LANES))
                o_v[rows, :] = jnp.where(lane8 < 64, total, summed)

    mine4 = pl.ds(s * 4, 4)
    for c in range(CHUNKS):
        wait_bytes(regs[c].at[pl.ds(0, 56)], zr.at[c])

        @pl.loop(0, LANES, unroll=8)
        def _(i):
            outgs[c][i] = regs[c][tab_s[0, i]]

        for o in PEERS:
            t = seq_peer(s, o)
            remote(outgs[c].at[pl.ds(t * 4, 4)], incs[c].at[mine4], xs.at[c], xr.at[c], {"seq": t}).start()
        incs[c][mine4] = outgs[c][mine4]
        kv_v[:, pl.ds(c * TOK, TOK), :] = regs[c][...]
        if c == LAG - 1:
            anchors()
        if c >= LAG:
            put(c - LAG)
        if c >= CHUNKS // 2:
            attend(0, range(c - CHUNKS // 2, c - CHUNKS // 2 + 1))

    attend(1, range(8))
    best = jnp.full((8, LANES), NEG_FILL, jnp.float32)

    def seq_max_step(p, best):
        top = jnp.maximum(m_v[page_rows(p), :], m_v[page_rows(64 + p), :])
        return jnp.maximum(best, jnp.where(memb_v[pl.ds(p, 1), :] > 0, top, NEG_FILL))

    best = lax.fori_loop(0, 64, seq_max_step, best, unroll=16)

    @pl.loop(0, 64, unroll=16)
    def _(p):
        inside = memb_v[pl.ds(p, 1), :] > 0
        for half in range(2):
            rows = page_rows(half * 64 + p)
            c_v[rows, :] = jnp.where(inside, jnp.exp(m_v[rows, :] - best), 0.0)

    bt_v[...] = jnp.concatenate([best] * 16, axis=0).T
    lane32 = iota((32, LANES), 1)
    stats = jnp.zeros((32, LANES), jnp.float32)
    for b in range(2):
        stats = jnp.where(
            (lane32 >> 3) == 2 + b, bt_v[pl.ds(b, 32, stride=2), :], stats
        )
    for j in range(8):
        coef = c_v[pl.ds(j, 128, stride=8), :]
        sums = o_v[pl.ds(j, 128, stride=8), :]
        rj_v[j] = lax.dot_general(
            coef.T, sums, (((1,), (0,)), ((), ())),
            precision=lax.Precision.HIGHEST, preferred_element_type=jnp.float32,
        )[0:64, :]
        even, odd = rj_v[j, pl.ds(0, 32, stride=2), :], rj_v[j, pl.ds(1, 32, stride=2), :]
        stats = jnp.where(lane32 == j, even[:, 0:1], stats)
        stats = jnp.where(lane32 == 8 + j, odd[:, 0:1], stats)
        ro_v[pl.ds(j, 32, stride=8), :] = jnp.where(lane32 < 64, pltpu.roll(even, 64, 1), odd)
    rm_v[:, 0, :] = stats

    for o in PEERS:
        t = seq_peer(s, o)
        remote(
            ro_v.at[pl.ds(pl.multiple_of(t * 8, 8), 8)], po_v.at[mine8], ps, pr, {"seq": t}
        ).start()
        remote(rm_v.at[t], pm_v.at[s], ms, mr, {"seq": t}).start()
    po_v[mine8, :] = ro_v[mine8, :]
    pm_v[s] = rm_v[s]

    for c in range(CHUNKS - LAG, CHUNKS):
        put(c)

    wait_bytes(pm_v.at[pl.ds(0, 31)], mr)
    turned = jnp.concatenate([pm_v[:, 0, :]] * 4, axis=0).T
    totals, tops = turned[0:16, :], turned[16:32, :]
    coef = jnp.exp(tops - jnp.max(tops, axis=1, keepdims=True))
    total = jnp.sum(jnp.where(iota((16, LANES), 1) < n_seq, coef * totals, 0.0), axis=1, keepdims=True)
    coef = coef / total
    wait_bytes(po_v.at[pl.ds(0, 248)], pr)
    acc = jnp.zeros((8, LANES), jnp.float32)
    for t in range(n_seq):
        part = jnp.where(lane8 < 64, coef[0:8, t : t + 1], coef[8:16, t : t + 1])
        acc = acc + part * po_v[t * 8 : (t + 1) * 8, :]
    turned = pltpu.roll(acc, 64, 1)
    low = lane1 < 64
    for k in range(4):
        first = jnp.where(low, acc[2 * k : 2 * k + 1], turned[2 * k + 1 : 2 * k + 2])
        second = jnp.where(low, turned[2 * k : 2 * k + 1], acc[2 * k + 1 : 2 * k + 2])
        both = jnp.concatenate([first, second], axis=0)
        att_v[:, k * LANES : (k + 1) * LANES] = both.astype(jnp.bfloat16)

    wait_bytes(dst_v.at[pl.ds(0, 56)], ds)
    wait_bytes(lab_in.at[pl.ds(0, 248)], ls)
    wait_bytes(po_v.at[pl.ds(0, 248)], ps)
    wait_bytes(pm_v.at[pl.ds(0, 31)], ms)
    for c in range(CHUNKS):
        wait_bytes(regs[c].at[pl.ds(0, 56)], zs.at[c])
        wait_bytes(incs[c].at[pl.ds(0, 124)], xs.at[c])


def write_out(cache_v, att_v, cache_hbm, att_hbm, sems):
    copies = [pltpu.make_async_copy(att_v, att_hbm, sems.at[8])]
    for i in range(8):
        pages = pl.ds(i * 8, 8)
        copies.append(pltpu.make_async_copy(cache_v.at[pages], cache_hbm.at[pages], sems.at[i]))
    for copy in copies:
        copy.start()
    for copy in copies:
        copy.wait()


def per_device(old_cache, page_dest, seq_pages, last_fill, queries):
    bf, f32, i32 = jnp.bfloat16, jnp.float32, jnp.int32
    vmem, dma = pltpu.VMEM, pltpu.SemaphoreType.DMA
    new_cache, att = pl.pallas_call(
        kernel,
        out_shape=(
            jax.ShapeDtypeStruct((64, 128, 128), bf),
            jax.ShapeDtypeStruct((2, 512), bf),
        ),
        in_specs=[pl.BlockSpec(memory_space=pltpu.HBM)] * 5,
        out_specs=(pl.BlockSpec(memory_space=pltpu.VMEM), pl.BlockSpec(memory_space=pltpu.VMEM)),
        scratch_shapes=[
            vmem((8, 8, 128, 128), bf),
            vmem((64, 512), bf),
            vmem((64, 8, LANES), f32),
            vmem((64, 128, 128), bf),
            pltpu.SMEM((8,), i32),
            pltpu.SMEM((64,), i32),
            pltpu.SMEM((64,), i32),
            vmem((64, LANES), i32),
            vmem((LANES, LANES), i32),
            vmem((256, LANES), i32),
            vmem((8, LANES), i32),
            pltpu.SMEM((8, LANES), i32),
            vmem((8, LANES), i32),
            pltpu.SMEM((8, LANES), i32),
            vmem((64, LANES), i32),
            vmem((64, LANES), f32),
            vmem((1024, LANES), f32),
            vmem((1024, LANES), f32),
            vmem((1024, LANES), f32),
            vmem((8, 64, LANES), f32),
            vmem((LANES, LANES), f32),
            vmem((256, LANES), f32),
            vmem((32, 1, LANES), f32),
            vmem((256, LANES), f32),
            vmem((32, 1, LANES), f32),
            [vmem((64, TOK, LANES), bf)] * CHUNKS,
            [vmem((128, TOK, LANES), bf)] * CHUNKS,
            [vmem((128, TOK, LANES), bf)] * CHUNKS,
            dma((CHUNKS,)), dma((CHUNKS,)), dma((CHUNKS,)), dma((CHUNKS,)),
            dma, dma, dma, dma, dma, dma, dma, dma, dma, dma((4,)), dma, dma,
        ],
        compiler_params=pltpu.CompilerParams(
            collective_id=0, has_side_effects=True, vmem_limit_bytes=50 * 2**20
        ),
    )(*[pltpu.with_memory_space_constraint(x, pltpu.HBM) for x in (old_cache, page_dest, seq_pages, last_fill, queries.reshape(64, 512))])
    new_cache, attended = pl.pallas_call(
        write_out,
        out_shape=(
            jax.ShapeDtypeStruct((64, 128, 128), bf),
            jax.ShapeDtypeStruct((2, 512), bf),
        ),
        in_specs=[pl.BlockSpec(memory_space=pltpu.VMEM)] * 2,
        out_specs=[pl.BlockSpec(memory_space=pltpu.HBM)] * 2,
        scratch_shapes=[dma((9,))],
        compiler_params=pltpu.CompilerParams(vmem_limit_bytes=50 * 2**20),
    )(new_cache, att)
    return new_cache.reshape(64, 1, 128, 128), attended.reshape(2, 1, 512)


def solution(mesh):
    in_specs = (
        P(("seq", "head"), None, None, None),
        P(("seq", "head")),
        P(),
        P(),
        P(None, "head", None),
    )
    out_specs = (P("seq", "head", None, None), P("seq", "head", None))
    return jax.shard_map(
        per_device, mesh=mesh, in_specs=in_specs, out_specs=out_specs, check_vma=False
    )
```
